32 devices in a mesh: dp: 4 (over z), stage: 2 (over y), tp: 4 (over x, core).
Axes of the slice: x: 2, y: 2, z: 4, core: 2. Of those that a mesh axis runs over, the one named last changes fastest.
Arguments:
- act_in: bfloat16 [2, 64, 14, 14, 512], P('stage', ('dp', 'tp'))
- conv_w: bfloat16 [2, 3, 3, 512, 1024], P('stage', None, None, 'tp')
- scale_vec: float32 [2, 1024], P('stage', 'tp')
- shift_vec: float32 [2, 1024], P('stage', 'tp')
- grad_z: bfloat16 [2, 64, 14, 14, 1024], P('stage', 'dp', None, None, 'tp')
Outputs:
- output 1: bfloat16 [2, 64, 14, 14, 1024], P('stage', 'dp', None, None, 'tp')
- output 2: bfloat16 [2, 64, 14, 14, 512], P('stage', ('dp', 'tp'))
- output 3: float32 [2, 3, 3, 512, 1024], P('stage', None, None, 'tp')
All inputs are finite; a program needn't handle non-finite values.
Results may differ from the reference program's by a relative error of at most 0.00771.
Values are sent between devices in bfloat16 or wider.
A program may use at most 1 GiB of HBM per device.

```python
import jax
import jax.numpy as jnp
from jax import lax

STAGES = 2
BATCH = 64
H = 14
W = 14
C = 512
CO = 1024


def place_stage(values, stage_index):
    pad_spec = [(stage_index, STAGES - 1 - stage_index)] + [(0, 0)] * values.ndim
    return jnp.pad(values[None], pad_spec)


def setup_inputs(seed: int = 0) -> dict:
    key = jax.random.key(seed)
    k_act, k_w, k_scale, k_sign, k_shift, k_grad = jax.random.split(key, 6)
    act_used = jax.random.normal(k_act, (BATCH, H, W, C), jnp.float32)
    w_used = jax.random.normal(k_w, (3, 3, C, CO), jnp.float32) * (9.0 * C) ** -0.5
    scale_sign = jnp.where(jax.random.randint(k_sign, (CO,), 0, 2) == 0, -1.0, 1.0)
    scale_used = scale_sign * jax.random.uniform(k_scale, (CO,), jnp.float32, 0.25, 1.75)
    shift_used = 0.8 * jax.random.normal(k_shift, (CO,), jnp.float32)
    grad_used = jax.random.normal(k_grad, (BATCH, H, W, CO), jnp.float32)
    return {
        "act_in": place_stage(act_used, 0).astype(jnp.bfloat16),
        "conv_w": place_stage(w_used, 1).astype(jnp.bfloat16),
        "scale_vec": place_stage(scale_used, 1),
        "shift_vec": place_stage(shift_used, 1),
        "grad_z": place_stage(grad_used, 1).astype(jnp.bfloat16),
    }


def conv_forward(images, kernel):
    return lax.conv_general_dilated(images, kernel, (1, 1), "SAME", dimension_numbers=("NHWC", "HWIO", "NHWC"))


def reference(act_in, conv_w, scale_vec, shift_vec, grad_z):
    kernel = conv_w[1].astype(jnp.float32)
    scale_one = scale_vec[1]
    shift_one = shift_vec[1]

    def one_image(dw_acc, img_pair):
        act_img, grad_img = img_pair
        image_f32 = act_img[None].astype(jnp.float32)
        pre_out, pull_back = jax.vjp(conv_forward, image_f32, kernel)
        lin_out = pre_out * scale_one + shift_one
        z_img = jnp.maximum(lin_out, 0.0).astype(jnp.bfloat16)
        grad_out = jnp.where(lin_out > 0, grad_img[None].astype(jnp.float32) * scale_one, 0.0).astype(jnp.bfloat16)
        dact_img, dw_img = pull_back(grad_out.astype(jnp.float32))
        return dw_acc + dw_img, (z_img[0], dact_img[0].astype(jnp.bfloat16))

    dw_init = jnp.zeros((3, 3, C, CO), jnp.float32)
    dw_sum, (z_used, dact_used) = lax.scan(one_image, dw_init, (act_in[0], grad_z[1]))
    return place_stage(z_used, 1), place_stage(dact_used, 0), place_stage(dw_sum, 1)
```

```python
import jax
import jax.numpy as jnp
from jax import lax
from jax.sharding import PartitionSpec as P


def conv_forward(images, kernel):
    return lax.conv_general_dilated(images, kernel, (1, 1), "SAME", dimension_numbers=("NHWC", "HWIO", "NHWC"), preferred_element_type=jnp.float32)


def conv_input_grad(grad_out, kernel):
    return lax.conv_general_dilated(grad_out, kernel[::-1, ::-1], (1, 1), "SAME", dimension_numbers=("NHWC", "HWOI", "NHWC"), preferred_element_type=jnp.float32)


def conv_kernel_grad(images, grad_out):
    return lax.conv_general_dilated(images, grad_out, (1, 1), ((1, 1), (1, 1)), dimension_numbers=("CHWN", "IHWO", "HWNC"), preferred_element_type=jnp.float32)


def solution(mesh):
    def body(act_loc, w_loc, scale_loc, shift_loc, grad_loc):
        t = lax.axis_index("tp")
        kernel = w_loc[0]
        moved = lax.ppermute(act_loc[0], "stage", perm=[(0, 1)])
        kernel_co = lax.all_to_all(kernel, "tp", 3, 2, tiled=True)
        act_all = lax.all_gather(moved, "tp", axis=0, tiled=True)
        pre_out = conv_forward(act_all, kernel_co)
        lin_out = pre_out * scale_loc[0] + shift_loc[0]
        z_blk = jnp.maximum(lin_out, 0.0).astype(jnp.bfloat16)
        grad_blk = jnp.where(lin_out > 0, grad_loc[0].astype(jnp.float32) * scale_loc[0], 0.0).astype(jnp.bfloat16)
        grad_full = lax.all_gather(grad_blk, "tp", axis=3, tiled=True)
        cc = kernel.shape[2]
        act_blk = lax.dynamic_slice_in_dim(act_all, t * cc, cc, axis=3)
        dw_part = conv_kernel_grad(act_blk, grad_full)
        dw_blk = lax.psum(dw_part, "dp")
        dact_blk = conv_input_grad(grad_full, kernel).astype(jnp.bfloat16)
        dact_back = lax.ppermute(dact_blk, "stage", perm=[(1, 0)])
        dact_img = lax.all_to_all(dact_back, "tp", 0, 3, tiled=True)
        return z_blk[None], dact_img[None], dw_blk[None]

    act_spec = P("stage", ("dp", "tp"))
    w_spec = P("stage", None, None, "tp")
    vec_spec = P("stage", "tp")
    grad_spec = P("stage", "dp", None, None, "tp")
    return jax.shard_map(body, mesh=mesh, in_specs=(act_spec, w_spec, vec_spec, vec_spec, grad_spec), out_specs=(grad_spec, act_spec, w_spec), check_vma=False)
```

```python
import jax
import jax.numpy as jnp
from jax import lax
from jax.experimental import pallas as pl
from jax.experimental.pallas import tpu as pltpu
from jax.sharding import PartitionSpec as P

BF = jnp.bfloat16
F32 = jnp.float32
HW = 14
NI = 16
PW = 16
CC = 128
CO = 256
CIN, COUT = 512, 1024
HC = 2
NH = HW // HC
NG = 4
GI = NI // NG
TAPS = 9
N1 = 5
N0 = TAPS - N1
LMID, LEND = 4, 9
ROWS = PW * NI
KROWS = HW * ROWS
KH = CC // 4


def copy_to(src, dst, ssem, rsem, dev):
    return pltpu.make_async_remote_copy(src, dst, ssem, rsem, device_id=dev, device_id_type=pl.DeviceIdType.MESH)


def loop(lo, hi, fn):
    def one(n, carry):
        fn(n)
        return carry

    lax.fori_loop(lo, hi, one, 0)


def body_kernel(
    act, w, sc, sh, dz, z_out, da_out, gw_out,
    IM, L, Kf, KX, Dv, AT, GP, PB, R1, R2, Kb, AC, DA, ZF,
    rA, sAy, sAx, sAc, rX, sXx, sXz, lK, sKc, rKc, lM, rG, sGx, sGc,
    rP, sP, r1, r2, s1, s2, s3, so, sU, rD, sD,
):
    z, y, t = lax.axis_index("dp"), lax.axis_index("stage"), lax.axis_index("tp")
    x, c = t // 2, t % 2
    tc = t + 1 - 2 * c
    tx = (t + 2) % NG
    txc = (tc + 2) % NG
    zp = z % 2
    dev_y, dev_x, dev_c = (z, 1 - y, t), (z, y, tx), (z, y, tc)
    dev_z = (z + 1 - 2 * zp, y, t)
    mid = (z == 1) | (z == 2)
    lag = jnp.where(mid, LMID, LEND)

    peers = [dev_x, dev_c, ((z + 1) % NG, y, t), ((z + 3) % NG, y, t)] + [(z, 1 - y, g) for g in (t, tc, tx, txc)]
    bar = pltpu.get_barrier_semaphore()
    for d in peers:
        pl.semaphore_signal(bar, 1, device_id=d, device_id_type=pl.DeviceIdType.MESH)
    pl.semaphore_wait(bar, len(peers))

    def lanes(start, size):
        return pl.ds(pl.multiple_of(start, CC), size)

    def rows(v):
        return pl.ds(HC * v, HC)

    def up1(q, p):
        return copy_to(PB.at[q, p], R1.at[q, p % N1], s1.at[q, p], r1.at[q, p], (z + 1, y, t))

    def from3(q, p):
        return copy_to(PB.at[q, p], R2.at[q, p], s1.at[q, p], r2.at[q, p], (z - 1, y, t))

    def root_lo(q, p):
        return copy_to(PB.at[q, p], R2.at[q, p], s2.at[q, p], r2.at[q, p], (z - 1, y, t))

    def root_hi(q, p):
        return copy_to(PB.at[q, p], R2.at[q, p], s3.at[q, p], r2.at[q, p], (z + 1, y, t))

    def last_lo(q, p):
        return copy_to(R2.at[q, p], R2.at[q, p], s2.at[q, p], r2.at[q, p], (z - 1, y, t))

    def reduce_end(q, p):
        @pl.when(z == 0)
        def _():
            up1(q, p).start()

        @pl.when(z == 3)
        def _():
            from3(q, p).start()

    def reduce_mid(q, p):
        @pl.when(z == 1)
        def _():
            up1(q, p).wait_recv()
            PB[q, p] = PB[q, p] + R1[q, p % N1]
            up1(q, p).start()

        @pl.when(z == 2)
        def _():
            up1(q, p).wait_recv()
            from3(q, p).wait_recv()
            PB[q, p] = PB[q, p] + R1[q, p % N1] + R2[q, p]
            root_lo(q, p).start()
            root_hi(q, p).start()

    def line_final(q, p, use):
        @pl.when(z != 2)
        def _():
            root_lo(q, p).wait_recv()

        @pl.when(z == 1)
        def _():
            last_lo(q, p).start()

        @pl.when(z == 2)
        def _():
            use(PB, q, p).start()

        @pl.when(z != 2)
        def _():
            use(R2, q, p).start()

    def line_drain(q, p):
        @pl.when(z != 2)
        def _():
            up1(q, p).wait_send()

        @pl.when(z == 2)
        def _():
            root_lo(q, p).wait_send()
            root_hi(q, p).wait_send()

        @pl.when(z == 1)
        def _():
            last_lo(q, p).wait_send()

    def down(q, p):
        return copy_to(PB.at[q, p], PB.at[q, p], sP.at[q, p], rP.at[q, p], dev_y)

    def up_final(src, q, p):
        return copy_to(src.at[q, p], R2.at[q, p], sU.at[q, p], r2.at[q, p], dev_y)

    def act_up(u):
        return copy_to(act.at[rows(u)], L.at[t, rows(u)], sAy.at[u], rA.at[t, u], dev_y)

    def da_land(src_t):
        return copy_to(
            DA.at[0], da_out.at[pl.ds(NH * (src_t % 2), NH), :, :, lanes(CO * (src_t // 2), CO)],
            sD.at[0], rD.at[src_t], dev_y)

    @pl.when(y == 0)
    def _():
        loop(0, NH, lambda u: act_up(u).start())
        ZF[...] = jnp.zeros(ZF.shape, F32)

        def zfill(n):
            return pltpu.make_async_copy(
                ZF, gw_out.at[n // NG, :, lanes(CO * (n % NG), CO)], so.at[n % NG, n // NG])

        loop(0, TAPS * NG, lambda n: zfill(n).start())

        def zero_row(h):
            Dv[h] = jnp.zeros(Dv.shape[1:], BF)

        loop(0, HW, zero_row)
        zc = pltpu.make_async_copy(Dv, z_out, lM.at[0])
        zc.start()

        def row_round(q0):
            cnt = 2 * N0

            def block(n):
                return q0 + n // N0, N1 + n % N0

            def step(n):
                @pl.when(n < cnt)
                def _():
                    q, p = block(n)
                    down(q, p).wait_recv()
                    reduce_end(q, p)
                    reduce_mid(q, p)

                @pl.when((n >= lag) & (n < cnt + lag))
                def _():
                    q, p = block(n - lag)
                    line_final(q, p, up_final)

            loop(0, cnt + LEND, step)

        row_round(0)
        row_round(2)

        def drain(n):
            q, p = n // N0, N1 + n % N0
            line_drain(q, p)
            up_final(R2, q, p).wait_send()

        loop(0, NG * N0, drain)
        loop(0, TAPS * NG, lambda n: zfill(n).wait())
        loop(0, NH, lambda u: act_up(u).wait_send())
        zc.wait()
        loop(0, NG, lambda g: da_land(g).wait_recv())

    @pl.when(y == 1)
    def _():
        def k_rows(b):
            return pl.ds(KH * b, KH)

        def kx_send(u):
            b = k_rows(2 * zp + u)
            return copy_to(w.at[:, b, lanes(2 * CO * (1 - x), 2 * CO)], KX.at[:, b, :], sXx.at[u], rX.at[2 * zp + u], dev_x)

        def kx_share(b, u):
            return copy_to(KX.at[:, k_rows(b), :], KX.at[:, k_rows(b), :], sXz.at[u], rX.at[b], dev_z)

        def kf_rows(chunk, b):
            return Kf.at[:, pl.ds(CC * chunk + KH * b, KH), :]

        def kx_mine(b):
            return pltpu.make_async_copy(KX.at[:, k_rows(b), lanes(CO * c, CO)], kf_rows(tx, b), lK.at[b])

        def kx_partner(b, chunk):
            return copy_to(KX.at[:, k_rows(b), lanes(CO * (1 - c), CO)], kf_rows(chunk, b), sKc.at[b], rKc.at[b], dev_c)

        def kx_got(b):
            kx_mine(b).start()
            kx_partner(b, tx).start()

        def kx_x(u):
            b = 2 * zp + u
            kx_share(b, u).wait_recv()
            kx_share(b, u).start()
            kx_got(b)

        def kx_z(u):
            b = 2 * (1 - zp) + u
            kx_share(b, u).wait_recv()
            kx_got(b)

        def k_part(chunk):
            return copy_to(w.at[:, :, lanes(CO * tc, CO)], Kf.at[:, pl.ds(CC * chunk, CC), :], sKc.at[4], rKc.at[4], dev_c)

        def kb_part(at):
            return copy_to(w, Kb.at[:, pl.ds(CC * at, CC), :], sKc.at[5], rKc.at[5], dev_c)

        for u in range(2):
            kx_send(u).start()
        k_own = pltpu.make_async_copy(w.at[:, :, lanes(CO * t, CO)], Kf.at[:, pl.ds(CC * t, CC), :], lK.at[4])
        k_own.start()
        k_part(t).start()
        kb_own = pltpu.make_async_copy(w, Kb.at[:, pl.ds(CC * c, CC), :], lM.at[1])
        kb_own.start()
        kb_part(c).start()
        d_load = pltpu.make_async_copy(dz, Dv, lM.at[2])
        d_load.start()

        def im_zero(h):
            IM[h, 0:2] = jnp.zeros((2, NI, CIN), BF)
            IM[h, PW:PW + 2] = jnp.zeros((2, NI, CIN), BF)

        loop(0, PW, im_zero)
        for h in (0, PW - 1):
            IM[h, 2:PW] = jnp.zeros((HW, NI, CIN), BF)
            AT[:, :, ROWS * h:ROWS * (h + 1)] = jnp.zeros((3, CC, ROWS), BF)

        def gp_zero(g):
            for h in (0, PW - 1):
                GP[g, h] = jnp.zeros((PW, NI, CO), BF)
                GP[g, :, h] = jnp.zeros((PW, NI, CO), BF)

        loop(0, NG, gp_zero)

        def a_x(u):
            return copy_to(L.at[t, rows(u)], L.at[t, rows(u)], sAx.at[u], rA.at[t, u], dev_x)

        def a_c(g, u, s):
            return copy_to(L.at[g, rows(u)], L.at[g, rows(u)], sAc.at[s, u], rA.at[g, u], dev_c)

        def a_wait(g, u):
            a_c(g, u, 0).wait_recv()

        def own_arrive(u):
            a_wait(t, u)
            a_x(u).start()
            a_c(t, u, 0).start()

        def x_arrive(u):
            a_wait(tx, u)
            a_c(tx, u, 1).start()

        def assemble(u):
            a_wait(tc, u)
            a_wait(txc, u)
            for hh in range(HC):
                h = HC * u + hh
                IM[h + 1, 2:PW] = jnp.concatenate([L[g, h] for g in range(NG)], axis=1)
                for j in range(3):
                    blk = IM[h + 1, j:j + PW, :, lanes(CC * t, CC)]
                    AT[j, :, pl.ds(pl.multiple_of(ROWS * (h + 1), ROWS), ROWS)] = blk.reshape(ROWS, CC).T

        def g_rows(co, v):
            return GP.at[co, pl.ds(HC * v + 1, HC), pl.ds(1, HW)]

        def g_x(v):
            return copy_to(g_rows(t, v), g_rows(t, v), sGx.at[v], rG.at[t, v], dev_x)

        def g_c(co, v, s):
            return copy_to(g_rows(co, v), g_rows(co, v), sGc.at[s, v], rG.at[co, v], dev_c)

        def g_wait(co, v):
            g_c(co, v, 0).wait_recv()

        scv, shv = sc[...].reshape(1, 1, 1, CO), sh[...].reshape(1, 1, 1, CO)

        def forward(v):
            def lhs(hh):
                return jnp.concatenate(
                    [IM[HC * v + hh + i, j + 1:j + 1 + HW].reshape(HW * NI, CIN) for i in range(3) for j in range(3)],
                    axis=1)

            pre = jnp.dot(
                jnp.concatenate([lhs(hh) for hh in range(HC)], axis=0),
                Kf[...].reshape(TAPS * CIN, CO), preferred_element_type=F32)
            lin = pre.reshape(HC, HW, NI, CO) * scv + shv
            dv = Dv[rows(v)].astype(F32)
            GP[t, pl.ds(HC * v + 1, HC), 1:1 + HW] = jnp.where(lin > 0, dv * scv, 0.0).astype(BF)
            Dv[rows(v)] = jnp.maximum(lin, 0.0).astype(BF)
            g_x(v).start()
            g_c(t, v, 0).start()

        own_arrive(0)
        own_arrive(1)
        kx_x(0)
        own_arrive(2)
        own_arrive(3)
        kx_x(1)
        own_arrive(4)
        own_arrive(5)
        kx_z(0)
        own_arrive(6)
        x_arrive(0)
        kx_z(1)
        x_arrive(1)
        assemble(0)
        x_arrive(2)
        assemble(1)
        k_own.wait()
        k_part(tc).wait_recv()
        for b in range(NG):
            kx_mine(b).wait()
            kx_partner(b, txc).wait_recv()
        d_load.wait()

        def pipe(u):
            @pl.when(u < NH)
            def _():
                x_arrive(u)

            assemble(u - 1)
            forward(u - 2)

        forward(0)
        loop(3, NH + 1, pipe)
        forward(NH - 1)
        zc = pltpu.make_async_copy(Dv, z_out, lM.at[0])
        zc.start()

        def gw_chunk(q, co):
            def part(j):
                lhs = jnp.concatenate([AT[j, :, ROWS * i:ROWS * i + KROWS] for i in range(3)], axis=0)
                r = jnp.dot(lhs, GP[co, 1:1 + HW].reshape(KROWS, CO), preferred_element_type=F32)
                for i in range(3):
                    PB[q, 3 * j + i] = r[CC * i:CC * (i + 1)]

            loop(0, 3, part)
            loop(0, N1, lambda p: reduce_end(q, p))
            loop(N1, TAPS, lambda p: down(q, p).start())

        def chunk_of(q):
            return (t + 2 * (q // 2) + (1 - 2 * c) * (q % 2) + NG) % NG

        def out_copy(src, q, p):
            tap = 3 * (p % 3) + p // 3
            return pltpu.make_async_copy(src.at[q, p], gw_out.at[tap, :, lanes(CO * chunk_of(q), CO)], so.at[q, p])

        def step(n):
            @pl.when(n < NG * N1)
            def _():
                reduce_mid(n // N1, n % N1)

            @pl.when((n >= lag) & (n < NG * N1 + lag))
            def _():
                m = n - lag
                line_final(m // N1, m % N1, out_copy)

        def da_tap(tap):
            i, j = tap // 3, tap % 3
            lhs = jnp.concatenate(
                [
                    GP[g, pl.ds(NH * c + 2 - i, NH), pl.ds(2 - j, HW)].reshape(NH * HW * NI, CO)
                    for g in range(NG)
                ],
                axis=1)
            return lax.dot_general(lhs, Kb[tap], (((1,), (1,)), ((), ())), preferred_element_type=F32)

        def da_send(g):
            return copy_to(
                DA.at[g], da_out.at[pl.ds(NH * c, NH), :, :, lanes(CO * x, CO)], sD.at[g], rD.at[t], (z, 0, g))

        gw_chunk(0, t)
        loop(0, NH, lambda v: g_wait(tc, v))
        gw_chunk(1, tc)

        def relay(v):
            g_wait(tx, v)
            g_c(tx, v, 1).start()

        n = 0
        for v in range(NH):
            relay(v)
            stop = n + 1 + v % 2
            loop(n, stop, step)
            n = stop
        gw_chunk(2, tx)
        loop(0, NH, lambda v: g_wait(txc, v))
        gw_chunk(3, txc)
        kb_own.wait()
        kb_part(1 - c).wait_recv()
        AC[...] = da_tap(0)

        def da_step(k):
            step(n + k - 1)
            AC[...] += da_tap(k)

        loop(1, TAPS, da_step)
        n = n + TAPS - 1
        for g in range(NG):
            DA[g] = AC[...].reshape(NH, HW, NI, CO)[:, :, GI * g:GI * (g + 1), :].astype(BF)
            da_send(g).start()
        loop(n, NG * N1 + LEND, step)

        def detour(m):
            q, p = m // N0, N1 + m % N0
            up_final(R2, q, p).wait_recv()
            out_copy(R2, q, p).start()

        loop(0, NG * N0, detour)

        for u in range(2):
            kx_send(u).wait_send()
            kx_share(2 * zp + u, u).wait_send()
        for b in range(NG):
            kx_partner(b, tx).wait_send()
        k_part(t).wait_send()
        kb_part(c).wait_send()

        def drain_a(u):
            a_x(u).wait_send()
            a_c(t, u, 0).wait_send()
            a_c(tx, u, 1).wait_send()
            g_x(u).wait_send()
            g_c(t, u, 0).wait_send()
            g_c(tx, u, 1).wait_send()

        loop(0, NH, drain_a)
        L[0] = jnp.zeros(L.shape[1:], BF)
        zeros = pltpu.make_async_copy(L.at[0], da_out, lM.at[3])
        zeros.start()
        loop(0, NG * N1, lambda m: line_drain(m // N1, m % N1))
        loop(0, NG * N0, lambda m: down(m // N0, N1 + m % N0).wait_send())
        loop(0, TAPS * NG, lambda m: out_copy(R2, m // TAPS, m % TAPS).wait())
        loop(0, NG, lambda g: da_send(g).wait_send())
        zc.wait()
        zeros.wait()


def solution(mesh):
    def body(act_loc, w_loc, scale_loc, shift_loc, grad_loc):
        dma = pltpu.SemaphoreType.DMA
        hbm = pl.BlockSpec(memory_space=pl.ANY)
        vmem = pl.BlockSpec(memory_space=pltpu.VMEM)
        block = (NG, TAPS)
        scratch = [
            pltpu.VMEM((PW, PW + 2, NI, CIN), BF),
            pltpu.VMEM((NG, HW, HW, GI, CIN), BF),
            pltpu.VMEM((TAPS, CIN, CO), BF),
            pltpu.VMEM((TAPS, CC, 2 * CO), BF),
            pltpu.VMEM((HW, HW, NI, CO), BF),
            pltpu.VMEM((3, CC, PW * ROWS), BF),
            pltpu.VMEM((NG, PW, PW, NI, CO), BF),
            pltpu.VMEM(block + (CC, CO), F32),
            pltpu.VMEM((NG, N1, CC, CO), F32),
            pltpu.VMEM(block + (CC, CO), F32),
            pltpu.VMEM((TAPS, 2 * CC, COUT), BF),
            pltpu.VMEM((NH * HW * NI, CO), F32),
            pltpu.VMEM((NG, NH, HW, GI, CO), BF),
            pltpu.VMEM((CC, CO), F32),
            dma((NG, NH)), dma((NH,)), dma((NH,)), dma((2, NH)),
            dma((4,)), dma((2,)), dma((2,)), dma((5,)), dma((6,)), dma((6,)), dma((4,)),
            dma((NG, NH)), dma((NH,)), dma((2, NH)),
        ] + [dma(block)] * 9 + [dma((NG,)), dma((NG,))]
        act = jnp.transpose(act_loc[0], (1, 2, 0, 3))
        dz = jnp.transpose(grad_loc[0], (1, 2, 0, 3))
        z_blk, da, gw = pl.pallas_call(
            body_kernel,
            out_shape=[
                jax.ShapeDtypeStruct((HW, HW, NI, CO), BF),
                jax.ShapeDtypeStruct((HW, HW, GI, CIN), BF),
                jax.ShapeDtypeStruct((TAPS, CC, COUT), F32),
            ],
            in_specs=[hbm, hbm, vmem, vmem, hbm],
            out_specs=[hbm, hbm, hbm],
            scratch_shapes=scratch,
            compiler_params=pltpu.CompilerParams(collective_id=0, has_side_effects=True, vmem_limit_bytes=62 * 2**20),
            name="stage_conv",
        )(act, w_loc[0].reshape(TAPS, CC, COUT), scale_loc, shift_loc, dz)
        back = (2, 0, 1, 3)
        return jnp.transpose(z_blk, back)[None], jnp.transpose(da, back)[None], gw.reshape(1, 3, 3, CC, COUT)

    act_spec = P("stage", ("dp", "tp"))
    w_spec = P("stage", None, None, "tp")
    vec_spec = P("stage", "tp")
    grad_spec = P("stage", "dp", None, None, "tp")
    return jax.shard_map(body, mesh=mesh, in_specs=(act_spec, w_spec, vec_spec, vec_spec, grad_spec), out_specs=(grad_spec, act_spec, w_spec), check_vma=False)
```

```python
import jax
import jax.numpy as jnp
from jax import lax
from jax.experimental import pallas as pl
from jax.experimental.pallas import tpu as pltpu
from jax.sharding import PartitionSpec as P

BF = jnp.bfloat16
F32 = jnp.float32
HW = 14
NI = 16
PW = 16
CC = 128
CO = 256
CIN, COUT = 512, 1024
HC = 2
NH = HW // HC
NG = 4
GI = NI // NG
TAPS = 9
NA, NB = 5, 6
NROW = 2 * NA + 2 * NB
NDET = NG * TAPS - NROW
LMID, LEND = 4, 9
ROWS = PW * NI
KROWS = HW * ROWS
KH = 16
KP = CC // KH
KHALF = KP // 2
UX = 3


def copy_to(src, dst, ssem, rsem, dev):
    return pltpu.make_async_remote_copy(src, dst, ssem, rsem, device_id=dev, device_id_type=pl.DeviceIdType.MESH)


def loop(lo, hi, fn):
    def one(n, carry):
        fn(n)
        return carry

    lax.fori_loop(lo, hi, one, 0)


def body_kernel(
    act, w, sc, sh, dz, z_out, da_out, gw_out,
    IM, L, Kf, KX, Dv, AT, GP, PB, R1, R2, Kb, AC, DA, ZF,
    rA, sAy, sAx, sAc, rX, sXx, sXz, lK, sKc, rKc, lM, rG, sGx, sGc,
    rP, sP, r1, r2, s1, s2, s3, so, sU, rD, sD,
):
    z, y, t = lax.axis_index("dp"), lax.axis_index("stage"), lax.axis_index("tp")
    x, c = t // 2, t % 2
    tc = t + 1 - 2 * c
    tx = (t + 2) % NG
    txc = (tc + 2) % NG
    zp = z % 2
    dev_y, dev_x, dev_c = (z, 1 - y, t), (z, y, tx), (z, y, tc)
    dev_z = (z + 1 - 2 * zp, y, t)
    mid = (z == 1) | (z == 2)
    lag = jnp.where(mid, LMID, LEND)

    peers = [dev_x, dev_c, ((z + 1) % NG, y, t), ((z + 3) % NG, y, t)] + [(z, 1 - y, g) for g in (t, tc, tx, txc)]
    bar = pltpu.get_barrier_semaphore()
    for d in peers:
        pl.semaphore_signal(bar, 1, device_id=d, device_id_type=pl.DeviceIdType.MESH)
    pl.semaphore_wait(bar, len(peers))

    def lanes(start, size):
        return pl.ds(pl.multiple_of(start, CC), size)

    def rows(v):
        return pl.ds(HC * v, HC)

    def row_block(n):
        m = n - 2 * NA
        late = m >= 0
        return jnp.where(late, 2 + m // NB, n // NA), jnp.where(late, m % NB, n % NA)

    def detour_block(n):
        m = n - 2 * (TAPS - NA)
        late = m >= 0
        lo, hi = TAPS - NA, TAPS - NB
        return jnp.where(late, 2 + m // hi, n // lo), jnp.where(late, NB + m % hi, NA + n % lo)

    def up1(q, p):
        return copy_to(PB.at[q, p], R1.at[q, p % NB], s1.at[q, p], r1.at[q, p], (z + 1, y, t))

    def from3(q, p):
        return copy_to(PB.at[q, p], R2.at[q, p], s1.at[q, p], r2.at[q, p], (z - 1, y, t))

    def root_lo(q, p):
        return copy_to(PB.at[q, p], R2.at[q, p], s2.at[q, p], r2.at[q, p], (z - 1, y, t))

    def root_hi(q, p):
        return copy_to(PB.at[q, p], R2.at[q, p], s3.at[q, p], r2.at[q, p], (z + 1, y, t))

    def last_lo(q, p):
        return copy_to(R2.at[q, p], R2.at[q, p], s2.at[q, p], r2.at[q, p], (z - 1, y, t))

    def reduce_end(q, p):
        @pl.when(z == 0)
        def _():
            up1(q, p).start()

        @pl.when(z == 3)
        def _():
            from3(q, p).start()

    def reduce_mid(q, p):
        @pl.when(z == 1)
        def _():
            up1(q, p).wait_recv()
            PB[q, p] = PB[q, p] + R1[q, p % NB]
            up1(q, p).start()

        @pl.when(z == 2)
        def _():
            up1(q, p).wait_recv()
            from3(q, p).wait_recv()
            PB[q, p] = PB[q, p] + R1[q, p % NB] + R2[q, p]
            root_lo(q, p).start()
            root_hi(q, p).start()

    def line_final(q, p, use):
        @pl.when(z != 2)
        def _():
            root_lo(q, p).wait_recv()

        @pl.when(z == 1)
        def _():
            last_lo(q, p).start()

        @pl.when(z == 2)
        def _():
            use(PB, q, p).start()

        @pl.when(z != 2)
        def _():
            use(R2, q, p).start()

    def line_drain(q, p):
        @pl.when(z != 2)
        def _():
            up1(q, p).wait_send()

        @pl.when(z == 2)
        def _():
            root_lo(q, p).wait_send()
            root_hi(q, p).wait_send()

        @pl.when(z == 1)
        def _():
            last_lo(q, p).wait_send()

    def down(q, p):
        return copy_to(PB.at[q, p], PB.at[q, p], sP.at[q, p], rP.at[q, p], dev_y)

    def up_final(src, q, p):
        return copy_to(src.at[q, p], R2.at[q, p], sU.at[q, p], r2.at[q, p], dev_y)

    def act_up(u):
        return copy_to(act.at[rows(u)], L.at[t, rows(u)], sAy.at[u], rA.at[t, u], dev_y)

    def act_cross(src_t, u):
        return copy_to(act.at[rows(u)], L.at[src_t, rows(u)], sAx.at[u], rA.at[src_t, u], dev_x)

    def act_relay(u):
        return copy_to(L.at[tx, rows(u)], L.at[tx, rows(u)], sAc.at[0, u], rA.at[tx, u], dev_y)

    def da_land(src_t):
        return copy_to(
            DA.at[0], da_out.at[pl.ds(NH * (src_t % 2), NH), :, :, lanes(CO * (src_t // 2), CO)],
            sD.at[0], rD.at[src_t], dev_y)

    @pl.when(y == 0)
    def _():
        loop(UX, NH, lambda u: act_up(u).start())
        loop(0, UX, lambda u: act_cross(t, u).start())

        def raise_rows(u):
            act_up(u).start()
            act_cross(tx, u).wait_recv()
            act_relay(u).start()

        loop(0, UX, raise_rows)
        ZF[...] = jnp.zeros(ZF.shape, F32)

        def zfill(n):
            return pltpu.make_async_copy(
                ZF, gw_out.at[n // NG, :, lanes(CO * (n % NG), CO)], so.at[n % NG, n // NG])

        loop(0, TAPS * NG, lambda n: zfill(n).start())

        def zero_row(h):
            Dv[h] = jnp.zeros(Dv.shape[1:], BF)

        loop(0, HW, zero_row)
        zc = pltpu.make_async_copy(Dv, z_out, lM.at[0])
        zc.start()

        def row_round(lo, hi):
            def step(n):
                @pl.when(n < hi)
                def _():
                    q, p = detour_block(n)
                    down(q, p).wait_recv()
                    reduce_end(q, p)
                    reduce_mid(q, p)

                @pl.when((n >= lo + lag) & (n < hi + lag))
                def _():
                    q, p = detour_block(n - lag)
                    line_final(q, p, up_final)

            loop(lo, hi + LEND, step)

        row_round(0, 2 * (TAPS - NA))
        row_round(2 * (TAPS - NA), NDET)

        def drain(n):
            q, p = detour_block(n)
            line_drain(q, p)
            up_final(R2, q, p).wait_send()

        loop(0, NDET, drain)
        loop(0, TAPS * NG, lambda n: zfill(n).wait())
        loop(0, NH, lambda u: act_up(u).wait_send())
        loop(0, UX, lambda u: act_cross(t, u).wait_send())
        loop(0, UX, lambda u: act_relay(u).wait_send())
        zc.wait()
        loop(0, NG, lambda g: da_land(g).wait_recv())

    @pl.when(y == 1)
    def _():
        def k_rows(b):
            return pl.ds(KH * b, KH)

        def kx_send(u):
            b = k_rows(KHALF * zp + u)
            return copy_to(w.at[:, b, lanes(2 * CO * (1 - x), 2 * CO)], KX.at[:, b, :], sXx.at[u], rX.at[KHALF * zp + u], dev_x)

        def kx_share(b, u):
            return copy_to(KX.at[:, k_rows(b), :], KX.at[:, k_rows(b), :], sXz.at[u], rX.at[b], dev_z)

        def kf_rows(chunk, b):
            return Kf.at[:, pl.ds(CC * chunk + KH * b, KH), :]

        def kx_mine(b):
            return pltpu.make_async_copy(KX.at[:, k_rows(b), lanes(CO * c, CO)], kf_rows(tx, b), lK.at[b])

        def kx_partner(b, chunk):
            return copy_to(KX.at[:, k_rows(b), lanes(CO * (1 - c), CO)], kf_rows(chunk, b), sKc.at[b], rKc.at[b], dev_c)

        def kx_got(b):
            kx_mine(b).start()
            kx_partner(b, tx).start()

        def kx_x(u):
            b = KHALF * zp + u
            kx_share(b, u).wait_recv()
            kx_share(b, u).start()
            kx_got(b)

        def kx_z(u):
            b = KHALF * (1 - zp) + u
            kx_share(b, u).wait_recv()
            kx_got(b)

        def k_part(chunk):
            return copy_to(w.at[:, :, lanes(CO * tc, CO)], Kf.at[:, pl.ds(CC * chunk, CC), :], sKc.at[KP], rKc.at[KP], dev_c)

        def kb_part(at):
            return copy_to(w, Kb.at[:, pl.ds(CC * at, CC), :], sKc.at[KP + 1], rKc.at[KP + 1], dev_c)

        loop(0, KHALF, lambda u: kx_send(u).start())
        k_own = pltpu.make_async_copy(w.at[:, :, lanes(CO * t, CO)], Kf.at[:, pl.ds(CC * t, CC), :], lK.at[KP])
        k_own.start()
        k_part(t).start()
        kb_own = pltpu.make_async_copy(w, Kb.at[:, pl.ds(CC * c, CC), :], lM.at[1])
        kb_own.start()
        kb_part(c).start()
        d_load = pltpu.make_async_copy(dz, Dv, lM.at[2])
        d_load.start()

        def im_zero(h):
            IM[h, 0:2] = jnp.zeros((2, NI, CIN), BF)
            IM[h, PW:PW + 2] = jnp.zeros((2, NI, CIN), BF)

        loop(0, PW, im_zero)
        for h in (0, PW - 1):
            IM[h, 2:PW] = jnp.zeros((HW, NI, CIN), BF)
            AT[:, :, ROWS * h:ROWS * (h + 1)] = jnp.zeros((3, CC, ROWS), BF)

        def gp_zero(g):
            for h in (0, PW - 1):
                GP[g, h] = jnp.zeros((PW, NI, CO), BF)
                GP[g, :, h] = jnp.zeros((PW, NI, CO), BF)

        loop(0, NG, gp_zero)

        def a_x(u):
            return copy_to(L.at[t, rows(u)], L.at[t, rows(u)], sAx.at[u], rA.at[t, u], dev_x)

        def a_c(g, u, s):
            return copy_to(L.at[g, rows(u)], L.at[g, rows(u)], sAc.at[s, u], rA.at[g, u], dev_c)

        def a_wait(g, u):
            a_c(g, u, 0).wait_recv()

        def own_arrive(u):
            a_wait(t, u)
            if u >= UX:
                a_x(u).start()
            a_c(t, u, 0).start()

        def x_arrive(u):
            a_wait(tx, u)
            a_c(tx, u, 1).start()

        def assemble(u):
            a_wait(tc, u)
            a_wait(txc, u)
            for hh in range(HC):
                h = HC * u + hh
                IM[h + 1, 2:PW] = jnp.concatenate([L[g, h] for g in range(NG)], axis=1)
                for j in range(3):
                    blk = IM[h + 1, j:j + PW, :, lanes(CC * t, CC)]
                    AT[j, :, pl.ds(pl.multiple_of(ROWS * (h + 1), ROWS), ROWS)] = blk.reshape(ROWS, CC).T

        def g_rows(co, v):
            return GP.at[co, pl.ds(HC * v + 1, HC), pl.ds(1, HW)]

        def g_x(v):
            return copy_to(g_rows(t, v), g_rows(t, v), sGx.at[v], rG.at[t, v], dev_x)

        def g_c(co, v, s):
            return copy_to(g_rows(co, v), g_rows(co, v), sGc.at[s, v], rG.at[co, v], dev_c)

        def g_wait(co, v):
            g_c(co, v, 0).wait_recv()

        scv, shv = sc[...].reshape(1, 1, 1, CO), sh[...].reshape(1, 1, 1, CO)

        def forward(v):
            def lhs(hh):
                return jnp.concatenate(
                    [IM[HC * v + hh + i, j + 1:j + 1 + HW].reshape(HW * NI, CIN) for i in range(3) for j in range(3)],
                    axis=1)

            pre = jnp.dot(
                jnp.concatenate([lhs(hh) for hh in range(HC)], axis=0),
                Kf[...].reshape(TAPS * CIN, CO), preferred_element_type=F32)
            lin = pre.reshape(HC, HW, NI, CO) * scv + shv
            dv = Dv[rows(v)].astype(F32)
            GP[t, pl.ds(HC * v + 1, HC), 1:1 + HW] = jnp.where(lin > 0, dv * scv, 0.0).astype(BF)
            Dv[rows(v)] = jnp.maximum(lin, 0.0).astype(BF)
            g_x(v).start()
            g_c(t, v, 0).start()

        own_arrive(3)
        kx_x(0)
        own_arrive(4)
        kx_x(1)
        own_arrive(5)
        kx_z(0)
        own_arrive(6)
        kx_x(2)
        kx_z(1)
        own_arrive(0)
        kx_x(3)
        x_arrive(0)
        kx_z(2)
        x_arrive(3)
        own_arrive(1)
        x_arrive(4)
        kx_z(3)
        assemble(3)
        assemble(0)
        k_own.wait()
        k_part(tc).wait_recv()

        def k_ready(b):
            kx_mine(b).wait()
            kx_partner(b, txc).wait_recv()

        loop(0, KP, k_ready)
        d_load.wait()
        x_arrive(1)
        assemble(4)
        assemble(1)
        forward(0)
        x_arrive(5)
        assemble(5)
        own_arrive(2)
        forward(4)
        x_arrive(6)
        assemble(6)
        x_arrive(2)
        loop(5, NH, forward)
        assemble(2)
        forward(3)
        loop(1, 3, forward)
        zc = pltpu.make_async_copy(Dv, z_out, lM.at[0])
        zc.start()

        def gw_chunk(q, co):
            mine = NA if q < 2 else NB

            def part(k):
                j = k if q < 2 else (k + 2) % 3
                lhs = jnp.concatenate([AT[j, :, ROWS * i:ROWS * i + KROWS] for i in range(3)], axis=0)
                r = jnp.dot(lhs, GP[co, 1:1 + HW].reshape(KROWS, CO), preferred_element_type=F32)
                for i in range(3):
                    p = 3 * j + i
                    PB[q, p] = r[CC * i:CC * (i + 1)]

                    @pl.when(p < mine)
                    def _():
                        reduce_end(q, p)

                    @pl.when(p >= mine)
                    def _():
                        down(q, p).start()

            loop(0, 3, part)

        def chunk_of(q):
            return (t + 2 * (q // 2) + (1 - 2 * c) * (q % 2) + NG) % NG

        def out_copy(src, q, p):
            tap = 3 * (p % 3) + p // 3
            return pltpu.make_async_copy(src.at[q, p], gw_out.at[tap, :, lanes(CO * chunk_of(q), CO)], so.at[q, p])

        def step(n):
            @pl.when(n < NROW)
            def _():
                reduce_mid(*row_block(n))

            @pl.when((n >= lag) & (n < NROW + lag))
            def _():
                q, p = row_block(n - lag)
                line_final(q, p, out_copy)

        def da_tap(tap):
            i, j = tap // 3, tap % 3
            lhs = jnp.concatenate(
                [
                    GP[g, pl.ds(NH * c + 2 - i, NH), pl.ds(2 - j, HW)].reshape(NH * HW * NI, CO)
                    for g in range(NG)
                ],
                axis=1)
            return lax.dot_general(lhs, Kb[tap], (((1,), (1,)), ((), ())), preferred_element_type=F32)

        def da_send(g):
            return copy_to(
                DA.at[g], da_out.at[pl.ds(NH * c, NH), :, :, lanes(CO * x, CO)], sD.at[g], rD.at[t], (z, 0, g))

        gw_chunk(0, t)
        loop(0, NH, lambda v: g_wait(tc, v))
        gw_chunk(1, tc)

        def relay(v):
            g_wait(tx, v)
            g_c(tx, v, 1).start()

        n = 0
        for v, stop in zip((0, 4, 5, 6, 3, 1, 2), (0, 0, 1, 3, 5, 7, 8)):
            relay(v)
            if stop > n:
                loop(n, stop, step)
            n = stop
        gw_chunk(2, tx)
        loop(0, NH, lambda v: g_wait(txc, v))
        gw_chunk(3, txc)
        kb_own.wait()
        kb_part(1 - c).wait_recv()
        AC[...] = da_tap(0)

        def da_step(k):
            step(n + k - 1)
            AC[...] += da_tap(k)

        loop(1, TAPS, da_step)
        n = n + TAPS - 1
        for g in range(NG):
            DA[g] = AC[...].reshape(NH, HW, NI, CO)[:, :, GI * g:GI * (g + 1), :].astype(BF)
            da_send(g).start()
        loop(n, NROW + LEND, step)

        def detour(m):
            q, p = detour_block(m)
            up_final(R2, q, p).wait_recv()
            out_copy(R2, q, p).start()

        loop(0, NDET, detour)

        loop(0, KHALF, lambda u: kx_send(u).wait_send())
        loop(0, KHALF, lambda u: kx_share(KHALF * zp + u, u).wait_send())
        loop(0, KP, lambda b: kx_partner(b, tx).wait_send())
        k_part(t).wait_send()
        kb_part(c).wait_send()

        def drain_a(u):
            a_c(t, u, 0).wait_send()
            a_c(tx, u, 1).wait_send()
            g_x(u).wait_send()
            g_c(t, u, 0).wait_send()
            g_c(tx, u, 1).wait_send()

        loop(0, NH, drain_a)
        loop(UX, NH, lambda u: a_x(u).wait_send())
        L[0] = jnp.zeros(L.shape[1:], BF)
        zeros = pltpu.make_async_copy(L.at[0], da_out, lM.at[3])
        zeros.start()
        loop(0, NROW, lambda m: line_drain(*row_block(m)))
        loop(0, NDET, lambda m: down(*detour_block(m)).wait_send())
        loop(0, TAPS * NG, lambda m: out_copy(R2, m // TAPS, m % TAPS).wait())
        loop(0, NG, lambda g: da_send(g).wait_send())
        zc.wait()
        zeros.wait()


def solution(mesh):
    def body(act_loc, w_loc, scale_loc, shift_loc, grad_loc):
        dma = pltpu.SemaphoreType.DMA
        hbm = pl.BlockSpec(memory_space=pl.ANY)
        vmem = pl.BlockSpec(memory_space=pltpu.VMEM)
        block = (NG, TAPS)
        scratch = [
            pltpu.VMEM((PW, PW + 2, NI, CIN), BF),
            pltpu.VMEM((NG, HW, HW, GI, CIN), BF),
            pltpu.VMEM((TAPS, CIN, CO), BF),
            pltpu.VMEM((TAPS, CC, 2 * CO), BF),
            pltpu.VMEM((HW, HW, NI, CO), BF),
            pltpu.VMEM((3, CC, PW * ROWS), BF),
            pltpu.VMEM((NG, PW, PW, NI, CO), BF),
            pltpu.VMEM(block + (CC, CO), F32),
            pltpu.VMEM((NG, NB, CC, CO), F32),
            pltpu.VMEM(block + (CC, CO), F32),
            pltpu.VMEM((TAPS, 2 * CC, COUT), BF),
            pltpu.VMEM((NH * HW * NI, CO), F32),
            pltpu.VMEM((NG, NH, HW, GI, CO), BF),
            pltpu.VMEM((CC, CO), F32),
            dma((NG, NH)), dma((NH,)), dma((NH,)), dma((2, NH)),
            dma((KP,)), dma((KHALF,)), dma((KHALF,)), dma((KP + 1,)), dma((KP + 2,)), dma((KP + 2,)), dma((4,)),
            dma((NG, NH)), dma((NH,)), dma((2, NH)),
        ] + [dma(block)] * 9 + [dma((NG,)), dma((NG,))]
        act = jnp.transpose(act_loc[0], (1, 2, 0, 3))
        dz = jnp.transpose(grad_loc[0], (1, 2, 0, 3))
        z_blk, da, gw = pl.pallas_call(
            body_kernel,
            out_shape=[
                jax.ShapeDtypeStruct((HW, HW, NI, CO), BF),
                jax.ShapeDtypeStruct((HW, HW, GI, CIN), BF),
                jax.ShapeDtypeStruct((TAPS, CC, COUT), F32),
            ],
            in_specs=[hbm, hbm, vmem, vmem, hbm],
            out_specs=[hbm, hbm, hbm],
            scratch_shapes=scratch,
            compiler_params=pltpu.CompilerParams(collective_id=0, has_side_effects=True, vmem_limit_bytes=62 * 2**20),
            name="stage_conv",
        )(act, w_loc[0].reshape(TAPS, CC, COUT), scale_loc, shift_loc, dz)
        back = (2, 0, 1, 3)
        return jnp.transpose(z_blk, back)[None], jnp.transpose(da, back)[None], gw.reshape(1, 3, 3, CC, COUT)

    act_spec = P("stage", ("dp", "tp"))
    w_spec = P("stage", None, None, "tp")
    vec_spec = P("stage", "tp")
    grad_spec = P("stage", "dp", None, None, "tp")
    return jax.shard_map(body, mesh=mesh, in_specs=(act_spec, w_spec, vec_spec, vec_spec, grad_spec), out_specs=(grad_spec, act_spec, w_spec), check_vma=False)
```

```python
import jax
import jax.numpy as jnp
from jax import lax
from jax.experimental import pallas as pl
from jax.experimental.pallas import tpu as pltpu
from jax.sharding import PartitionSpec as P

BF = jnp.bfloat16
F32 = jnp.float32
HW = 14
NI = 16
PW = 16
CC = 128
CO = 256
CIN, COUT = 512, 1024
HC = 2
NH = HW // HC
NG = 4
GI = NI // NG
TAPS = 9
NA, NB = 5, 5
NROW = 2 * NA + 2 * NB
NDET = NG * TAPS - NROW
LMID, LEND, LEND0 = 3, 8, 6
ROWS = PW * NI
KROWS = HW * ROWS
KH = 16
KP = CC // KH
KHALF = KP // 2
UX = 3


def copy_to(src, dst, ssem, rsem, dev):
    return pltpu.make_async_remote_copy(src, dst, ssem, rsem, device_id=dev, device_id_type=pl.DeviceIdType.MESH)


def loop(lo, hi, fn):
    def one(n, carry):
        fn(n)
        return carry

    lax.fori_loop(lo, hi, one, 0)


def body_kernel(
    act, w, sc, sh, dz, z_out, da_out, gw_out,
    IM, L, Kf, KX, Dv, AT, GP, PB, R1, R2, Kb, AC, DA, ZF,
    rA, sAy, sAx, sAc, rX, sXx, sXz, lK, sKc, rKc, lM, rG, sGx, sGc,
    rP, sP, r1, r2, s1, s2, s3, so, sU, rD, sD,
):
    z, y, t = lax.axis_index("dp"), lax.axis_index("stage"), lax.axis_index("tp")
    x, c = t // 2, t % 2
    tc = t + 1 - 2 * c
    tx = (t + 2) % NG
    txc = (tc + 2) % NG
    zp = z % 2
    dev_y, dev_x, dev_c = (z, 1 - y, t), (z, y, tx), (z, y, tc)
    dev_z = (z + 1 - 2 * zp, y, t)
    mid = (z == 1) | (z == 2)
    lag = jnp.where(mid, LMID, LEND)

    peers = [dev_x, dev_c, ((z + 1) % NG, y, t), ((z + 3) % NG, y, t)] + [(z, 1 - y, g) for g in (t, tc, tx, txc)]
    bar = pltpu.get_barrier_semaphore()
    for d in peers:
        pl.semaphore_signal(bar, 1, device_id=d, device_id_type=pl.DeviceIdType.MESH)
    pl.semaphore_wait(bar, len(peers))

    def lanes(start, size):
        return pl.ds(pl.multiple_of(start, CC), size)

    def rows(v):
        return pl.ds(HC * v, HC)

    def row_block(n):
        m = n - 2 * NA
        late = m >= 0
        return jnp.where(late, 2 + m // NB, n // NA), jnp.where(late, (m + 3) % NB, n % NA)

    def detour_block(n):
        m = n - 2 * (TAPS - NA)
        late = m >= 0
        lo, hi = TAPS - NA, TAPS - NB
        return jnp.where(late, 2 + m // hi, n // lo), jnp.where(late, NB + (m + 1) % hi, NA + n % lo)

    def up1(q, p):
        return copy_to(PB.at[q, p], R1.at[q, p % NB], s1.at[q, p], r1.at[q, p], (z + 1, y, t))

    def from3(q, p):
        return copy_to(PB.at[q, p], R2.at[q, p], s1.at[q, p], r2.at[q, p], (z - 1, y, t))

    def root_lo(q, p):
        return copy_to(PB.at[q, p], R2.at[q, p], s2.at[q, p], r2.at[q, p], (z - 1, y, t))

    def root_hi(q, p):
        return copy_to(PB.at[q, p], R2.at[q, p], s3.at[q, p], r2.at[q, p], (z + 1, y, t))

    def last_lo(q, p):
        return copy_to(R2.at[q, p], R2.at[q, p], s2.at[q, p], r2.at[q, p], (z - 1, y, t))

    def reduce_end(q, p):
        @pl.when(z == 0)
        def _():
            up1(q, p).start()

        @pl.when(z == 3)
        def _():
            from3(q, p).start()

    def reduce_mid(q, p):
        @pl.when(z == 1)
        def _():
            up1(q, p).wait_recv()
            PB[q, p] = PB[q, p] + R1[q, p % NB]
            up1(q, p).start()

        @pl.when(z == 2)
        def _():
            up1(q, p).wait_recv()
            from3(q, p).wait_recv()
            PB[q, p] = PB[q, p] + R1[q, p % NB] + R2[q, p]
            root_lo(q, p).start()
            root_hi(q, p).start()

    def line_final(q, p, use):
        @pl.when(z != 2)
        def _():
            root_lo(q, p).wait_recv()

        @pl.when(z == 1)
        def _():
            last_lo(q, p).start()

        @pl.when(z == 2)
        def _():
            use(PB, q, p).start()

        @pl.when(z != 2)
        def _():
            use(R2, q, p).start()

    def line_drain(q, p):
        @pl.when(z != 2)
        def _():
            up1(q, p).wait_send()

        @pl.when(z == 2)
        def _():
            root_lo(q, p).wait_send()
            root_hi(q, p).wait_send()

        @pl.when(z == 1)
        def _():
            last_lo(q, p).wait_send()

    def down(q, p):
        return copy_to(PB.at[q, p], PB.at[q, p], sP.at[q, p], rP.at[q, p], dev_y)

    def up_final(src, q, p):
        return copy_to(src.at[q, p], R2.at[q, p], sU.at[q, p], r2.at[q, p], dev_y)

    def act_up(u):
        return copy_to(act.at[rows(u)], L.at[t, rows(u)], sAy.at[u], rA.at[t, u], dev_y)

    def act_cross(src_t, u):
        return copy_to(act.at[rows(u)], L.at[src_t, rows(u)], sAx.at[u], rA.at[src_t, u], dev_x)

    def act_relay(u):
        return copy_to(L.at[tx, rows(u)], L.at[tx, rows(u)], sAc.at[0, u], rA.at[tx, u], dev_y)

    def da_land(src_t):
        return copy_to(
            DA.at[0], da_out.at[pl.ds(NH * (src_t % 2), NH), :, :, lanes(CO * (src_t // 2), CO)],
            sD.at[0], rD.at[src_t], dev_y)

    @pl.when(y == 0)
    def _():
        loop(0, UX, lambda u: act_up(u).start())
        loop(UX, NH, lambda u: act_cross(t, u).start())

        def raise_rows(u):
            act_up(u).start()
            act_cross(tx, u).wait_recv()
            act_relay(u).start()

        loop(UX, NH, raise_rows)
        ZF[...] = jnp.zeros(ZF.shape, F32)

        def zfill(n):
            return pltpu.make_async_copy(
                ZF, gw_out.at[n // NG, :, lanes(CO * (n % NG), CO)], so.at[n % NG, n // NG])

        loop(0, TAPS * NG, lambda n: zfill(n).start())

        def zero_row(h):
            Dv[h] = jnp.zeros(Dv.shape[1:], BF)

        loop(0, HW, zero_row)
        zc = pltpu.make_async_copy(Dv, z_out, lM.at[0])
        zc.start()

        lag0 = jnp.where(mid, LMID, LEND0)

        def step0(n):
            @pl.when(n < NDET)
            def _():
                q, p = detour_block(n)
                down(q, p).wait_recv()
                reduce_end(q, p)
                reduce_mid(q, p)

            @pl.when((n >= lag0) & (n < NDET + lag0))
            def _():
                q, p = detour_block(n - lag0)
                line_final(q, p, up_final)

        loop(0, NDET + LEND0, step0)

        def drain(n):
            q, p = detour_block(n)
            line_drain(q, p)
            up_final(R2, q, p).wait_send()

        loop(0, NDET, drain)
        loop(0, TAPS * NG, lambda n: zfill(n).wait())
        loop(0, NH, lambda u: act_up(u).wait_send())
        loop(UX, NH, lambda u: act_cross(t, u).wait_send())
        loop(UX, NH, lambda u: act_relay(u).wait_send())
        zc.wait()
        loop(0, NG, lambda g: da_land(g).wait_recv())

    @pl.when(y == 1)
    def _():
        def k_rows(b):
            return pl.ds(KH * b, KH)

        def kx_send(u):
            b = k_rows(KHALF * zp + u)
            return copy_to(w.at[:, b, lanes(2 * CO * (1 - x), 2 * CO)], KX.at[:, b, :], sXx.at[u], rX.at[KHALF * zp + u], dev_x)

        def kx_share(b, u):
            return copy_to(KX.at[:, k_rows(b), :], KX.at[:, k_rows(b), :], sXz.at[u], rX.at[b], dev_z)

        def kf_rows(chunk, b):
            return Kf.at[:, pl.ds(CC * chunk + KH * b, KH), :]

        def kx_mine(b):
            return pltpu.make_async_copy(KX.at[:, k_rows(b), lanes(CO * c, CO)], kf_rows(tx, b), lK.at[b])

        def kx_partner(b, chunk):
            return copy_to(KX.at[:, k_rows(b), lanes(CO * (1 - c), CO)], kf_rows(chunk, b), sKc.at[b], rKc.at[b], dev_c)

        def kx_got(b):
            kx_mine(b).start()
            kx_partner(b, tx).start()

        def kx_x(u):
            b = KHALF * zp + u
            kx_share(b, u).wait_recv()
            kx_share(b, u).start()
            kx_got(b)

        def kx_z(u):
            b = KHALF * (1 - zp) + u
            kx_share(b, u).wait_recv()
            kx_got(b)

        def k_part(chunk):
            return copy_to(w.at[:, :, lanes(CO * tc, CO)], Kf.at[:, pl.ds(CC * chunk, CC), :], sKc.at[KP], rKc.at[KP], dev_c)

        def kb_part(at):
            return copy_to(w, Kb.at[:, pl.ds(CC * at, CC), :], sKc.at[KP + 1], rKc.at[KP + 1], dev_c)

        loop(0, KHALF, lambda u: kx_send(u).start())
        k_own = pltpu.make_async_copy(w.at[:, :, lanes(CO * t, CO)], Kf.at[:, pl.ds(CC * t, CC), :], lK.at[KP])
        k_own.start()
        k_part(t).start()
        kb_own = pltpu.make_async_copy(w, Kb.at[:, pl.ds(CC * c, CC), :], lM.at[1])
        kb_own.start()
        kb_part(c).start()
        d_load = pltpu.make_async_copy(dz, Dv, lM.at[2])
        d_load.start()

        def im_zero(h):
            IM[h, 0:2] = jnp.zeros((2, NI, CIN), BF)
            IM[h, PW:PW + 2] = jnp.zeros((2, NI, CIN), BF)

        loop(0, PW, im_zero)
        for h in (0, PW - 1):
            IM[h, 2:PW] = jnp.zeros((HW, NI, CIN), BF)
            AT[:, :, ROWS * h:ROWS * (h + 1)] = jnp.zeros((3, CC, ROWS), BF)

        def gp_zero(g):
            for h in (0, PW - 1):
                GP[g, h] = jnp.zeros((PW, NI, CO), BF)
                GP[g, :, h] = jnp.zeros((PW, NI, CO), BF)

        loop(0, NG, gp_zero)

        def a_x(u):
            return copy_to(L.at[t, rows(u)], L.at[t, rows(u)], sAx.at[u], rA.at[t, u], dev_x)

        def a_c(g, u, s):
            return copy_to(L.at[g, rows(u)], L.at[g, rows(u)], sAc.at[s, u], rA.at[g, u], dev_c)

        def a_wait(g, u):
            a_c(g, u, 0).wait_recv()

        def own_arrive(u):
            a_wait(t, u)
            if u < UX:
                a_x(u).start()
            a_c(t, u, 0).start()

        def x_arrive(u):
            a_wait(tx, u)
            a_c(tx, u, 1).start()

        def assemble(u):
            a_wait(tc, u)
            a_wait(txc, u)
            for hh in range(HC):
                h = HC * u + hh
                IM[h + 1, 2:PW] = jnp.concatenate([L[g, h] for g in range(NG)], axis=1)
                for j in range(3):
                    blk = IM[h + 1, j:j + PW, :, lanes(CC * t, CC)]
                    AT[j, :, pl.ds(pl.multiple_of(ROWS * (h + 1), ROWS), ROWS)] = blk.reshape(ROWS, CC).T

        def g_rows(co, v):
            return GP.at[co, pl.ds(HC * v + 1, HC), pl.ds(1, HW)]

        def g_x(v):
            return copy_to(g_rows(t, v), g_rows(t, v), sGx.at[v], rG.at[t, v], dev_x)

        def g_c(co, v, s):
            return copy_to(g_rows(co, v), g_rows(co, v), sGc.at[s, v], rG.at[co, v], dev_c)

        def g_wait(co, v):
            g_c(co, v, 0).wait_recv()

        scv, shv = sc[...].reshape(1, 1, 1, CO), sh[...].reshape(1, 1, 1, CO)

        def forward(v):
            def lhs(hh):
                return jnp.concatenate(
                    [IM[HC * v + hh + i, j + 1:j + 1 + HW].reshape(HW * NI, CIN) for i in range(3) for j in range(3)],
                    axis=1)

            pre = jnp.dot(
                jnp.concatenate([lhs(hh) for hh in range(HC)], axis=0),
                Kf[...].reshape(TAPS * CIN, CO), preferred_element_type=F32)
            lin = pre.reshape(HC, HW, NI, CO) * scv + shv
            dv = Dv[rows(v)].astype(F32)
            GP[t, pl.ds(HC * v + 1, HC), 1:1 + HW] = jnp.where(lin > 0, dv * scv, 0.0).astype(BF)
            Dv[rows(v)] = jnp.maximum(lin, 0.0).astype(BF)
            g_x(v).start()
            g_c(t, v, 0).start()

        own_arrive(0)
        kx_x(0)
        own_arrive(1)
        kx_x(1)
        own_arrive(2)
        kx_z(0)
        kx_x(2)
        own_arrive(3)
        kx_z(1)
        x_arrive(3)
        kx_x(3)
        own_arrive(4)
        kx_z(2)
        x_arrive(0)
        x_arrive(4)
        x_arrive(1)
        assemble(3)
        assemble(0)
        kx_z(3)
        own_arrive(5)
        x_arrive(2)
        assemble(4)
        assemble(1)
        k_own.wait()
        k_part(tc).wait_recv()

        def k_ready(b):
            kx_mine(b).wait()
            kx_partner(b, txc).wait_recv()

        loop(0, KP, k_ready)
        d_load.wait()
        forward(0)
        x_arrive(5)
        assemble(2)
        forward(1)
        own_arrive(6)
        loop(2, 4, forward)
        x_arrive(6)
        assemble(5)
        forward(4)
        assemble(6)
        loop(5, NH, forward)
        zc = pltpu.make_async_copy(Dv, z_out, lM.at[0])
        zc.start()

        def gw_chunk(q, co, first=None):
            mine = NA if q < 2 else NB

            def part(k):
                j = k if q < 2 else 2 - k
                lhs = jnp.concatenate([AT[j, :, ROWS * i:ROWS * i + KROWS] for i in range(3)], axis=0)
                r = jnp.dot(lhs, GP[co, 1:1 + HW].reshape(KROWS, CO), preferred_element_type=F32)
                for i in range(3):
                    p = 3 * j + i
                    PB[q, p] = r[CC * i:CC * (i + 1)]

                    @pl.when(p < mine)
                    def _():
                        reduce_end(q, p)

                    @pl.when(p >= mine)
                    def _():
                        down(q, p).start()

            def part_step(k):
                part(k)
                if q == 2:

                    @pl.when(k > 0)
                    def _():
                        step(first + k - 1)

                if q == 3:
                    step(first + k)

            loop(0, 3, part_step)

        def chunk_of(q):
            return (t + 2 * (q // 2) + (1 - 2 * c) * (q % 2) + NG) % NG

        def out_copy(src, q, p):
            tap = 3 * (p % 3) + p // 3
            return pltpu.make_async_copy(src.at[q, p], gw_out.at[tap, :, lanes(CO * chunk_of(q), CO)], so.at[q, p])

        def step(n):
            @pl.when(n < NROW)
            def _():
                reduce_mid(*row_block(n))

            @pl.when((n >= lag) & (n < NROW + lag))
            def _():
                q, p = row_block(n - lag)
                line_final(q, p, out_copy)

        def da_tap(tap):
            i, j = tap // 3, tap % 3
            lhs = jnp.concatenate(
                [
                    GP[g, pl.ds(NH * c + 2 - i, NH), pl.ds(2 - j, HW)].reshape(NH * HW * NI, CO)
                    for g in range(NG)
                ],
                axis=1)
            return lax.dot_general(lhs, Kb[tap], (((1,), (1,)), ((), ())), preferred_element_type=F32)

        def da_send(g):
            return copy_to(
                DA.at[g], da_out.at[pl.ds(NH * c, NH), :, :, lanes(CO * x, CO)], sD.at[g], rD.at[t], (z, 0, g))

        gw_chunk(0, t)
        loop(0, NH, lambda v: g_wait(tc, v))
        gw_chunk(1, tc)

        def relay(v):
            g_wait(tx, v)
            g_c(tx, v, 1).start()

        n = 0
        for v, stop in enumerate((0, 0, 1, 3, 4, 6, 2 * NA)):
            relay(v)
            if stop > n:
                loop(n, stop, step)
            n = stop
        gw_chunk(2, tx, n)
        loop(0, NH, lambda v: g_wait(txc, v))
        gw_chunk(3, txc, n + 2)
        n = n + 5
        kb_own.wait()
        kb_part(1 - c).wait_recv()
        AC[...] = da_tap(0)

        def da_step(k):
            step(n + k)
            AC[...] += da_tap(2 * k + 1) + da_tap(2 * k + 2)

        loop(0, TAPS // 2, da_step)
        n = n + TAPS // 2
        for g in range(NG):
            DA[g] = AC[...].reshape(NH, HW, NI, CO)[:, :, GI * g:GI * (g + 1), :].astype(BF)
            da_send(g).start()
        loop(n, NROW + LEND, step)

        def detour(m):
            q, p = detour_block(m)
            up_final(R2, q, p).wait_recv()
            out_copy(R2, q, p).start()

        loop(0, NDET, detour)

        loop(0, KHALF, lambda u: kx_send(u).wait_send())
        loop(0, KHALF, lambda u: kx_share(KHALF * zp + u, u).wait_send())
        loop(0, KP, lambda b: kx_partner(b, tx).wait_send())
        k_part(t).wait_send()
        kb_part(c).wait_send()

        def drain_a(u):
            a_c(t, u, 0).wait_send()
            a_c(tx, u, 1).wait_send()
            g_x(u).wait_send()
            g_c(t, u, 0).wait_send()
            g_c(tx, u, 1).wait_send()

        loop(0, NH, drain_a)
        loop(0, UX, lambda u: a_x(u).wait_send())
        L[0] = jnp.zeros(L.shape[1:], BF)
        zeros = pltpu.make_async_copy(L.at[0], da_out, lM.at[3])
        zeros.start()
        loop(0, NROW, lambda m: line_drain(*row_block(m)))
        loop(0, NDET, lambda m: down(*detour_block(m)).wait_send())
        loop(0, TAPS * NG, lambda m: out_copy(R2, m // TAPS, m % TAPS).wait())
        loop(0, NG, lambda g: da_send(g).wait_send())
        zc.wait()
        zeros.wait()


def solution(mesh):
    def body(act_loc, w_loc, scale_loc, shift_loc, grad_loc):
        dma = pltpu.SemaphoreType.DMA
        hbm = pl.BlockSpec(memory_space=pl.ANY)
        vmem = pl.BlockSpec(memory_space=pltpu.VMEM)
        block = (NG, TAPS)
        scratch = [
            pltpu.VMEM((PW, PW + 2, NI, CIN), BF),
            pltpu.VMEM((NG, HW, HW, GI, CIN), BF),
            pltpu.VMEM((TAPS, CIN, CO), BF),
            pltpu.VMEM((TAPS, CC, 2 * CO), BF),
            pltpu.VMEM((HW, HW, NI, CO), BF),
            pltpu.VMEM((3, CC, PW * ROWS), BF),
            pltpu.VMEM((NG, PW, PW, NI, CO), BF),
            pltpu.VMEM(block + (CC, CO), F32),
            pltpu.VMEM((NG, NB, CC, CO), F32),
            pltpu.VMEM(block + (CC, CO), F32),
            pltpu.VMEM((TAPS, 2 * CC, COUT), BF),
            pltpu.VMEM((NH * HW * NI, CO), F32),
            pltpu.VMEM((NG, NH, HW, GI, CO), BF),
            pltpu.VMEM((CC, CO), F32),
            dma((NG, NH)), dma((NH,)), dma((NH,)), dma((2, NH)),
            dma((KP,)), dma((KHALF,)), dma((KHALF,)), dma((KP + 1,)), dma((KP + 2,)), dma((KP + 2,)), dma((4,)),
            dma((NG, NH)), dma((NH,)), dma((2, NH)),
        ] + [dma(block)] * 9 + [dma((NG,)), dma((NG,))]
        act = jnp.transpose(act_loc[0], (1, 2, 0, 3))
        dz = jnp.transpose(grad_loc[0], (1, 2, 0, 3))
        z_blk, da, gw = pl.pallas_call(
            body_kernel,
            out_shape=[
                pltpu.VMEM((HW, HW, NI, CO), BF),
                pltpu.VMEM((HW, HW, GI, CIN), BF),
                pltpu.VMEM((TAPS, CC, COUT), F32),
            ],
            in_specs=[hbm, hbm, vmem, vmem, hbm],
            out_specs=[vmem, vmem, vmem],
            scratch_shapes=scratch,
            compiler_params=pltpu.CompilerParams(collective_id=0, has_side_effects=True, vmem_limit_bytes=54 * 2**20),
            name="stage_conv",
        )(act, w_loc[0].reshape(TAPS, CC, COUT), scale_loc, shift_loc, dz)
        back = (2, 0, 1, 3)
        return jnp.transpose(z_blk, back)[None], jnp.transpose(da, back)[None], gw.reshape(1, 3, 3, CC, COUT)

    act_spec = P("stage", ("dp", "tp"))
    w_spec = P("stage", None, None, "tp")
    vec_spec = P("stage", "tp")
    grad_spec = P("stage", "dp", None, None, "tp")
    return jax.shard_map(body, mesh=mesh, in_specs=(act_spec, w_spec, vec_spec, vec_spec, grad_spec), out_specs=(grad_spec, act_spec, w_spec), check_vma=False)
```

```python
import jax
import jax.numpy as jnp
from jax import lax
from jax.experimental import pallas as pl
from jax.experimental.pallas import tpu as pltpu
from jax.sharding import PartitionSpec as P

BF = jnp.bfloat16
F32 = jnp.float32
HW = 14
NI = 16
PW = 16
CC = 128
CO = 256
CIN, COUT = 512, 1024
HC = 2
NH = HW // HC
NG = 4
GI = NI // NG
TAPS = 9
NA, NB = 4, 6
NROW = 2 * NA + 2 * NB
NDET = NG * TAPS - NROW
LMID, LEND, LEND0 = 3, 8, 5
ROWS = PW * NI
KROWS = HW * ROWS
KH = 16
KP = CC // KH
KHALF = KP // 2
UX = 3


def copy_to(src, dst, ssem, rsem, dev):
    return pltpu.make_async_remote_copy(src, dst, ssem, rsem, device_id=dev, device_id_type=pl.DeviceIdType.MESH)


def loop(lo, hi, fn):
    def one(n, carry):
        fn(n)
        return carry

    lax.fori_loop(lo, hi, one, 0)


def body_kernel(
    act, w, sc, sh, dz, z_out, da_out, gw_out,
    IM, L, Kf, KX, Dv, AT, GP, PB, R1, R2, Kb, AC, DA,
    rA, sAy, sAx, sAc, rX, sXx, sXz, lK, sKc, rKc, lM, rG, sGx, sGc,
    rP, sP, r1, r2, s1, s2, s3, sU, rD, sD,
):
    z, y, t = lax.axis_index("dp"), lax.axis_index("stage"), lax.axis_index("tp")
    x, c = t // 2, t % 2
    tc = t + 1 - 2 * c
    tx = (t + 2) % NG
    txc = (tc + 2) % NG
    zp = z % 2
    dev_y, dev_x, dev_c = (z, 1 - y, t), (z, y, tx), (z, y, tc)
    dev_z = (z + 1 - 2 * zp, y, t)
    mid = (z == 1) | (z == 2)
    lag = jnp.where(mid, LMID, LEND)

    peers = [dev_x, dev_c, ((z + 1) % NG, y, t), ((z + 3) % NG, y, t)] + [(z, 1 - y, g) for g in (t, tc, tx, txc)]
    bar = pltpu.get_barrier_semaphore()
    for d in peers:
        pl.semaphore_signal(bar, 1, device_id=d, device_id_type=pl.DeviceIdType.MESH)
    pl.semaphore_wait(bar, len(peers))

    def lanes(start, size):
        return pl.ds(pl.multiple_of(start, CC), size)

    def rows(v):
        return pl.ds(HC * v, HC)

    def row_block(n):
        m = n - 2 * NA
        late = m >= 0
        return jnp.where(late, 2 + m // NB, n // NA), jnp.where(late, (m + 3) % NB, n % NA)

    def detour_block(n):
        m = n - 2 * (TAPS - NA)
        late = m >= 0
        lo, hi = TAPS - NA, TAPS - NB
        return jnp.where(late, 2 + m // hi, n // lo), jnp.where(late, NB + (m + 1) % hi, NA + n % lo)

    def up1(q, p):
        return copy_to(PB.at[q, p], R1.at[q, p % NB], s1.at[q, p], r1.at[q, p], (z + 1, y, t))

    def from3(q, p):
        return copy_to(PB.at[q, p], R2.at[q, p], s1.at[q, p], r2.at[q, p], (z - 1, y, t))

    def root_lo(q, p):
        return copy_to(PB.at[q, p], R2.at[q, p], s2.at[q, p], r2.at[q, p], (z - 1, y, t))

    def root_hi(q, p):
        return copy_to(PB.at[q, p], R2.at[q, p], s3.at[q, p], r2.at[q, p], (z + 1, y, t))

    def last_lo(q, p):
        return copy_to(R2.at[q, p], R2.at[q, p], s2.at[q, p], r2.at[q, p], (z - 1, y, t))

    def reduce_end(q, p):
        @pl.when(z == 0)
        def _():
            up1(q, p).start()

        @pl.when(z == 3)
        def _():
            from3(q, p).start()

    def reduce_mid(q, p):
        @pl.when(z == 1)
        def _():
            up1(q, p).wait_recv()
            PB[q, p] = PB[q, p] + R1[q, p % NB]
            up1(q, p).start()

        @pl.when(z == 2)
        def _():
            up1(q, p).wait_recv()
            from3(q, p).wait_recv()
            PB[q, p] = PB[q, p] + R1[q, p % NB] + R2[q, p]
            root_lo(q, p).start()
            root_hi(q, p).start()

    def line_final(q, p, use):
        @pl.when(z != 2)
        def _():
            root_lo(q, p).wait_recv()

        @pl.when(z == 1)
        def _():
            last_lo(q, p).start()

        @pl.when(z == 2)
        def _():
            use(PB, q, p)

        @pl.when(z != 2)
        def _():
            use(R2, q, p)

    def line_drain(q, p):
        @pl.when(z != 2)
        def _():
            up1(q, p).wait_send()

        @pl.when(z == 2)
        def _():
            root_lo(q, p).wait_send()
            root_hi(q, p).wait_send()

        @pl.when(z == 1)
        def _():
            last_lo(q, p).wait_send()

    def down(q, p):
        return copy_to(PB.at[q, p], PB.at[q, p], sP.at[q, p], rP.at[q, p], dev_y)

    def up_final(src, q, p):
        return copy_to(src.at[q, p], R2.at[q, p], sU.at[q, p], r2.at[q, p], dev_y)

    def act_up(u):
        return copy_to(act.at[rows(u)], L.at[t, rows(u)], sAy.at[u], rA.at[t, u], dev_y)

    def act_cross(src_t, u):
        return copy_to(act.at[rows(u)], L.at[src_t, rows(u)], sAx.at[u], rA.at[src_t, u], dev_x)

    def act_relay(u):
        return copy_to(L.at[tx, rows(u)], L.at[tx, rows(u)], sAc.at[0, u], rA.at[tx, u], dev_y)

    def da_land(src_t):
        return copy_to(
            DA.at[0], da_out.at[pl.ds(NH * (src_t % 2), NH), :, :, lanes(CO * (src_t // 2), CO)],
            sD.at[0], rD.at[src_t], dev_y)

    @pl.when(y == 0)
    def _():
        loop(0, UX, lambda u: act_up(u).start())
        loop(UX, NH, lambda u: act_cross(t, u).start())

        def raise_rows(u):
            act_up(u).start()
            act_cross(tx, u).wait_recv()
            act_relay(u).start()

        loop(UX, NH, raise_rows)
        def no_grad_w(tap):
            gw_out[tap] = jnp.zeros((CC, COUT), F32)

        def no_z(h):
            z_out[h] = jnp.zeros((HW, NI, CO), BF)

        loop(0, TAPS, no_grad_w)
        loop(0, HW, no_z)
        lag0 = jnp.where(mid, LMID, LEND0)

        def step0(n):
            @pl.when(n < NDET)
            def _():
                q, p = detour_block(n)
                down(q, p).wait_recv()
                reduce_end(q, p)
                reduce_mid(q, p)

            @pl.when((n >= lag0) & (n < NDET + lag0))
            def _():
                q, p = detour_block(n - lag0)
                line_final(q, p, lambda src, q, p: up_final(src, q, p).start())

        loop(0, NDET + LEND0, step0)

        def drain(n):
            q, p = detour_block(n)
            line_drain(q, p)
            up_final(R2, q, p).wait_send()

        loop(0, NDET, drain)
        loop(0, NH, lambda u: act_up(u).wait_send())
        loop(UX, NH, lambda u: act_cross(t, u).wait_send())
        loop(UX, NH, lambda u: act_relay(u).wait_send())
        loop(0, NG, lambda g: da_land(g).wait_recv())

    @pl.when(y == 1)
    def _():
        def k_rows(b):
            return pl.ds(KH * b, KH)

        def kx_send(u):
            b = k_rows(KHALF * zp + u)
            return copy_to(w.at[:, b, lanes(2 * CO * (1 - x), 2 * CO)], KX.at[:, b, :], sXx.at[u], rX.at[KHALF * zp + u], dev_x)

        def kx_share(b, u):
            return copy_to(KX.at[:, k_rows(b), :], KX.at[:, k_rows(b), :], sXz.at[u], rX.at[b], dev_z)

        def kf_rows(chunk, b):
            return Kf.at[:, pl.ds(CC * chunk + KH * b, KH), :]

        def kx_mine(b):
            return pltpu.make_async_copy(KX.at[:, k_rows(b), lanes(CO * c, CO)], kf_rows(tx, b), lK.at[b])

        def kx_partner(b, chunk):
            return copy_to(KX.at[:, k_rows(b), lanes(CO * (1 - c), CO)], kf_rows(chunk, b), sKc.at[b], rKc.at[b], dev_c)

        def kx_got(b):
            kx_mine(b).start()
            kx_partner(b, tx).start()

        def kx_x(u):
            b = KHALF * zp + u
            kx_share(b, u).wait_recv()
            kx_share(b, u).start()
            kx_got(b)

        def kx_z(u):
            b = KHALF * (1 - zp) + u
            kx_share(b, u).wait_recv()
            kx_got(b)

        def k_part(chunk):
            return copy_to(w.at[:, :, lanes(CO * tc, CO)], Kf.at[:, pl.ds(CC * chunk, CC), :], sKc.at[KP], rKc.at[KP], dev_c)

        def kb_part(at):
            return copy_to(w, Kb.at[:, pl.ds(CC * at, CC), :], sKc.at[KP + 1], rKc.at[KP + 1], dev_c)

        loop(0, KHALF, lambda u: kx_send(u).start())
        k_own = pltpu.make_async_copy(w.at[:, :, lanes(CO * t, CO)], Kf.at[:, pl.ds(CC * t, CC), :], lK.at[KP])
        k_own.start()
        k_part(t).start()
        kb_own = pltpu.make_async_copy(w, Kb.at[:, pl.ds(CC * c, CC), :], lM.at[1])
        kb_own.start()
        kb_part(c).start()
        d_load = pltpu.make_async_copy(dz, Dv, lM.at[2])
        d_load.start()

        def im_zero(h):
            IM[h, 0:2] = jnp.zeros((2, NI, CIN), BF)
            IM[h, PW:PW + 2] = jnp.zeros((2, NI, CIN), BF)

        loop(0, PW, im_zero)
        for h in (0, PW - 1):
            IM[h, 2:PW] = jnp.zeros((HW, NI, CIN), BF)
            AT[:, :, ROWS * h:ROWS * (h + 1)] = jnp.zeros((3, CC, ROWS), BF)

        def gp_zero(g):
            for h in (0, PW - 1):
                GP[g, h] = jnp.zeros((PW, NI, CO), BF)
                GP[g, :, h] = jnp.zeros((PW, NI, CO), BF)

        loop(0, NG, gp_zero)

        def no_grad_act(h):
            da_out[h] = jnp.zeros((HW, GI, CIN), BF)

        loop(0, HW, no_grad_act)

        def a_x(u):
            return copy_to(L.at[t, rows(u)], L.at[t, rows(u)], sAx.at[u], rA.at[t, u], dev_x)

        def a_c(g, u, s):
            return copy_to(L.at[g, rows(u)], L.at[g, rows(u)], sAc.at[s, u], rA.at[g, u], dev_c)

        def a_wait(g, u):
            a_c(g, u, 0).wait_recv()

        def own_arrive(u):
            a_wait(t, u)
            if u < UX:
                a_x(u).start()
            a_c(t, u, 0).start()

        def x_arrive(u):
            a_wait(tx, u)
            a_c(tx, u, 1).start()

        def assemble(u):
            a_wait(tc, u)
            a_wait(txc, u)
            for hh in range(HC):
                h = HC * u + hh
                IM[h + 1, 2:PW] = jnp.concatenate([L[g, h] for g in range(NG)], axis=1)
                for j in range(3):
                    blk = IM[h + 1, j:j + PW, :, lanes(CC * t, CC)]
                    AT[j, :, pl.ds(pl.multiple_of(ROWS * (h + 1), ROWS), ROWS)] = blk.reshape(ROWS, CC).T

        def g_rows(co, v):
            return GP.at[co, pl.ds(HC * v + 1, HC), pl.ds(1, HW)]

        def g_x(v):
            return copy_to(g_rows(t, v), g_rows(t, v), sGx.at[v], rG.at[t, v], dev_x)

        def g_c(co, v, s):
            return copy_to(g_rows(co, v), g_rows(co, v), sGc.at[s, v], rG.at[co, v], dev_c)

        def g_wait(co, v):
            g_c(co, v, 0).wait_recv()

        scv, shv = sc[...].reshape(1, 1, 1, CO), sh[...].reshape(1, 1, 1, CO)

        def forward(v):
            def lhs(hh):
                return jnp.concatenate(
                    [IM[HC * v + hh + i, j + 1:j + 1 + HW].reshape(HW * NI, CIN) for i in range(3) for j in range(3)],
                    axis=1)

            pre = jnp.dot(
                jnp.concatenate([lhs(hh) for hh in range(HC)], axis=0),
                Kf[...].reshape(TAPS * CIN, CO), preferred_element_type=F32)
            lin = pre.reshape(HC, HW, NI, CO) * scv + shv
            dv = Dv[rows(v)].astype(F32)
            GP[t, pl.ds(HC * v + 1, HC), 1:1 + HW] = jnp.where(lin > 0, dv * scv, 0.0).astype(BF)
            z_out[rows(v)] = jnp.maximum(lin, 0.0).astype(BF)
            g_x(v).start()
            g_c(t, v, 0).start()

        own_arrive(0)
        kx_x(0)
        own_arrive(1)
        kx_x(1)
        own_arrive(2)
        kx_z(0)
        kx_x(2)
        own_arrive(3)
        kx_z(1)
        x_arrive(3)
        kx_x(3)
        own_arrive(4)
        kx_z(2)
        x_arrive(0)
        x_arrive(4)
        x_arrive(1)
        assemble(3)
        assemble(0)
        kx_z(3)
        own_arrive(5)
        x_arrive(2)
        assemble(4)
        assemble(1)
        k_own.wait()
        k_part(tc).wait_recv()

        def k_ready(b):
            kx_mine(b).wait()
            kx_partner(b, txc).wait_recv()

        loop(0, KP, k_ready)
        d_load.wait()
        forward(0)
        x_arrive(5)
        assemble(2)
        forward(1)
        own_arrive(6)
        loop(2, 4, forward)
        x_arrive(6)
        assemble(5)
        forward(4)
        assemble(6)
        loop(5, NH, forward)

        def gw_chunk(q, co, first=None):
            mine = NA if q < 2 else NB

            def part(k):
                j = k if q < 2 else 2 - k
                lhs = jnp.concatenate([AT[j, :, ROWS * i:ROWS * i + KROWS] for i in range(3)], axis=0)
                r = jnp.dot(lhs, GP[co, 1:1 + HW].reshape(KROWS, CO), preferred_element_type=F32)
                for i in range(3):
                    p = 3 * j + i
                    PB[q, p] = r[CC * i:CC * (i + 1)]

                    @pl.when(p < mine)
                    def _():
                        reduce_end(q, p)

                    @pl.when(p >= mine)
                    def _():
                        down(q, p).start()

            def part_step(k):
                part(k)
                if q == 2:

                    @pl.when(k > 0)
                    def _():
                        step(first + k - 1)

                if q == 3:
                    step(first + k)

            loop(0, 3, part_step)

        def chunk_of(q):
            return (t + 2 * (q // 2) + (1 - 2 * c) * (q % 2) + NG) % NG

        def put(src, q, p):
            tap = 3 * (p % 3) + p // 3
            gw_out[tap, :, lanes(CO * chunk_of(q), CO)] = src[q, p]

        def step(n):
            @pl.when(n < NROW)
            def _():
                reduce_mid(*row_block(n))

            @pl.when((n >= lag) & (n < NROW + lag))
            def _():
                q, p = row_block(n - lag)
                line_final(q, p, put)

        def da_tap(tap):
            i, j = tap // 3, tap % 3
            lhs = jnp.concatenate(
                [
                    GP[g, pl.ds(NH * c + 2 - i, NH), pl.ds(2 - j, HW)].reshape(NH * HW * NI, CO)
                    for g in range(NG)
                ],
                axis=1)
            return lax.dot_general(lhs, Kb[tap], (((1,), (1,)), ((), ())), preferred_element_type=F32)

        def da_send(g):
            return copy_to(
                DA.at[g], da_out.at[pl.ds(NH * c, NH), :, :, lanes(CO * x, CO)], sD.at[g], rD.at[t], (z, 0, g))

        gw_chunk(0, t)
        loop(0, NH, lambda v: g_wait(tc, v))
        gw_chunk(1, tc)

        def relay(v):
            g_wait(tx, v)
            g_c(tx, v, 1).start()

        n = 0
        for v, stop in enumerate((0, 0, 1, 3, 4, 6, 2 * NA)):
            relay(v)
            if stop > n:
                loop(n, stop, step)
            n = stop
        gw_chunk(2, tx, n)
        loop(0, NH, lambda v: g_wait(txc, v))
        gw_chunk(3, txc, n + 2)
        n = n + 5
        kb_own.wait()
        kb_part(1 - c).wait_recv()
        AC[...] = da_tap(0)

        def da_step(k):
            step(n + k)
            AC[...] += da_tap(2 * k + 1) + da_tap(2 * k + 2)

        loop(0, TAPS // 2, da_step)
        n = n + TAPS // 2
        for g in range(NG):
            DA[g] = AC[...].reshape(NH, HW, NI, CO)[:, :, GI * g:GI * (g + 1), :].astype(BF)
            da_send(g).start()
        loop(n, NROW + LEND, step)

        def detour(m):
            q, p = detour_block(m)
            up_final(R2, q, p).wait_recv()
            put(R2, q, p)

        loop(0, NDET, detour)

        loop(0, KHALF, lambda u: kx_send(u).wait_send())
        loop(0, KHALF, lambda u: kx_share(KHALF * zp + u, u).wait_send())
        loop(0, KP, lambda b: kx_partner(b, tx).wait_send())
        k_part(t).wait_send()
        kb_part(c).wait_send()

        def drain_a(u):
            a_c(t, u, 0).wait_send()
            a_c(tx, u, 1).wait_send()
            g_x(u).wait_send()
            g_c(t, u, 0).wait_send()
            g_c(tx, u, 1).wait_send()

        loop(0, NH, drain_a)
        loop(0, UX, lambda u: a_x(u).wait_send())
        loop(0, NROW, lambda m: line_drain(*row_block(m)))
        loop(0, NDET, lambda m: down(*detour_block(m)).wait_send())
        loop(0, NG, lambda g: da_send(g).wait_send())


def solution(mesh):
    def body(act_loc, w_loc, scale_loc, shift_loc, grad_loc):
        dma = pltpu.SemaphoreType.DMA
        hbm = pl.BlockSpec(memory_space=pl.ANY)
        vmem = pl.BlockSpec(memory_space=pltpu.VMEM)
        block = (NG, TAPS)
        scratch = [
            pltpu.VMEM((PW, PW + 2, NI, CIN), BF),
            pltpu.VMEM((NG, HW, HW, GI, CIN), BF),
            pltpu.VMEM((TAPS, CIN, CO), BF),
            pltpu.VMEM((TAPS, CC, 2 * CO), BF),
            pltpu.VMEM((HW, HW, NI, CO), BF),
            pltpu.VMEM((3, CC, PW * ROWS), BF),
            pltpu.VMEM((NG, PW, PW, NI, CO), BF),
            pltpu.VMEM(block + (CC, CO), F32),
            pltpu.VMEM((NG, NB, CC, CO), F32),
            pltpu.VMEM(block + (CC, CO), F32),
            pltpu.VMEM((TAPS, 2 * CC, COUT), BF),
            pltpu.VMEM((NH * HW * NI, CO), F32),
            pltpu.VMEM((NG, NH, HW, GI, CO), BF),
            dma((NG, NH)), dma((NH,)), dma((NH,)), dma((2, NH)),
            dma((KP,)), dma((KHALF,)), dma((KHALF,)), dma((KP + 1,)), dma((KP + 2,)), dma((KP + 2,)), dma((4,)),
            dma((NG, NH)), dma((NH,)), dma((2, NH)),
        ] + [dma(block)] * 8 + [dma((NG,)), dma((NG,))]
        act = jnp.transpose(act_loc[0], (1, 2, 0, 3))
        dz = jnp.transpose(grad_loc[0], (1, 2, 0, 3))
        z_blk, da, gw = pl.pallas_call(
            body_kernel,
            out_shape=[
                pltpu.VMEM((HW, HW, NI, CO), BF),
                pltpu.VMEM((HW, HW, GI, CIN), BF),
                pltpu.VMEM((TAPS, CC, COUT), F32),
            ],
            in_specs=[hbm, hbm, vmem, vmem, hbm],
            out_specs=[vmem, vmem, vmem],
            scratch_shapes=scratch,
            compiler_params=pltpu.CompilerParams(collective_id=0, has_side_effects=True, vmem_limit_bytes=54 * 2**20),
            name="stage_conv",
        )(act, w_loc[0].reshape(TAPS, CC, COUT), scale_loc, shift_loc, dz)
        back = (2, 0, 1, 3)
        return jnp.transpose(z_blk, back)[None], jnp.transpose(da, back)[None], gw.reshape(1, 3, 3, CC, COUT)

    act_spec = P("stage", ("dp", "tp"))
    w_spec = P("stage", None, None, "tp")
    vec_spec = P("stage", "tp")
    grad_spec = P("stage", "dp", None, None, "tp")
    return jax.shard_map(body, mesh=mesh, in_specs=(act_spec, w_spec, vec_spec, vec_spec, grad_spec), out_specs=(grad_spec, act_spec, w_spec), check_vma=False)
```
